32 devices in a mesh: dp: 2 (over z, core), tp: 16 (over x, y).
Axes of the slice: x: 4, y: 4, z: 1, core: 2. Of those that a mesh axis runs over, the one named last changes fastest.
The devices are a block of a 4x4x8 slice.
Arguments:
- x: bfloat16 [256, 3072], P('dp'), parts along dimension 0
- w_gate: bfloat16 [3072, 24576], P(None, 'tp')
- w_up: bfloat16 [3072, 24576], P(None, 'tp')
- w_down: bfloat16 [24576, 3072], P('tp')
Outputs:
- output: bfloat16 [256, 3072], P('dp'), parts along dimension 0
There are 2 independent parts. The reference program is written for one: setup_inputs(seed, part) draws one part's arguments, and reference() takes and returns one part's arrays. A program takes and returns all parts, laid end to end along the dimension named above; an argument that names none is the same for every part.
All inputs are finite; a program needn't handle non-finite values.
Results may differ from the reference program's by a relative error of at most 0.016.
Values are sent between devices in bfloat16 or wider.
A program may use at most 768 MiB of HBM per device.

```python
import jax
import jax.numpy as jnp

ROWS = 128
D = 3072
FF = 24576


def setup_inputs(seed: int = 0, part: int = 0) -> dict:
    kx, kg, ku, kd = jax.random.split(jax.random.key(seed), 4)
    drawn = {
        "x": jax.random.normal(jax.random.fold_in(kx, part), (ROWS, D), jnp.float32),
        "w_gate": jax.random.normal(kg, (D, FF), jnp.float32) * D**-0.5,
        "w_up": jax.random.normal(ku, (D, FF), jnp.float32) * D**-0.5,
        "w_down": jax.random.normal(kd, (FF, D), jnp.float32) * FF**-0.5,
    }
    return {k: v.astype(jnp.bfloat16) for k, v in drawn.items()}


def reference(x, w_gate, w_up, w_down):
    gate = jnp.dot(x, w_gate, preferred_element_type=jnp.float32)
    up = jnp.dot(x, w_up, preferred_element_type=jnp.float32)
    hidden = (jax.nn.gelu(gate) * up).astype(jnp.bfloat16)
    return jnp.dot(hidden, w_down, preferred_element_type=jnp.float32).astype(jnp.bfloat16)
```

```python
import functools
import math

import jax
import jax.numpy as jnp
from jax import lax
from jax.experimental import pallas as pl
from jax.experimental.pallas import tpu as pltpu
from jax.sharding import PartitionSpec as P

F32, BF16 = jnp.float32, jnp.bfloat16
MESH = pl.DeviceIdType.MESH
SLICES = 3
BLOCK = 256


def _kernel(side, x_hbm, wg_hbm, wu_hbm, wd_hbm, y, xv, wg, wu, wd, hid, term, send, part, psum, pout, p2, local_sem, ssem, rsem):
    me = lax.axis_index("tp")
    pos = (me // side, me % side)
    rows, depth = x_hbm.shape
    units = wg_hbm.shape[1]
    cw = send.shape[-1]
    span = side * cw
    quarter = rows // side

    def peer(axis, d):
        p = list(pos)
        p[axis] = lax.rem(p[axis] + d, side)
        return p[0] * side + p[1]

    barrier = pltpu.get_barrier_semaphore()
    for axis in (0, 1):
        for d in range(1, side):
            pl.semaphore_signal(barrier, inc=1, device_id={"tp": peer(axis, d)}, device_id_type=MESH)

    blocks = units // BLOCK
    cx = pltpu.make_async_copy(x_hbm, xv, local_sem.at[0])
    cx.start()
    cg, cu, cd = [], [], []
    for j in range(blocks):
        cols = pl.ds(j * BLOCK, BLOCK)
        cg.append(pltpu.make_async_copy(wg_hbm.at[:, cols], wg.at[j], local_sem.at[1 + j]))
        cu.append(pltpu.make_async_copy(wu_hbm.at[:, cols], wu.at[j], local_sem.at[1 + blocks + j]))
        cg[j].start()
        cu[j].start()
    for i in range(2 * SLICES):
        cd.append(pltpu.make_async_copy(wd_hbm.at[:, pl.ds(i * span, span)], wd.at[i], local_sem.at[1 + 2 * blocks + i]))
        cd[i].start()

    cx.wait()
    for j in range(blocks):
        cg[j].wait()
        gate = jnp.dot(xv[...], wg[j], preferred_element_type=F32)
        cu[j].wait()
        up = jnp.dot(xv[...], wu[j], preferred_element_type=F32)
        hid[:, j * BLOCK : (j + 1) * BLOCK] = (jax.nn.gelu(gate) * up).astype(BF16)

    def column(s, h, t):
        return pl.ds(pl.multiple_of((2 * s + h) * span + t * cw, cw), cw)

    def copy(stage, s, h, d, src, dst):
        axis = h if stage in (0, 3) else 1 - h
        i = ((s * 2 + h) * 4 + stage) * (side - 1) + d - 1
        return pltpu.make_async_remote_copy(
            src_ref=src,
            dst_ref=dst,
            send_sem=ssem.at[i],
            recv_sem=rsem.at[i],
            device_id={"tp": peer(axis, d)},
            device_id_type=MESH,
        )

    def copies(stage, s, h):
        mine, other = pos[h], pos[1 - h]
        out = []
        for d in range(1, side):
            if stage == 0:
                c = copy(0, s, h, d, send.at[s, h, lax.rem(mine + d, side)], part.at[s, h, d - 1])
            elif stage == 1:
                to = pl.multiple_of(lax.rem(other + d, side) * quarter, quarter)
                c = copy(1, s, h, d, pout.at[s, h, pl.ds(to, quarter)], p2.at[s, h, d - 1])
            elif stage == 2:
                block = y.at[pl.ds(pl.multiple_of(other * quarter, quarter), quarter), column(s, h, mine)]
                c = copy(2, s, h, d, block, block)
            else:
                block = y.at[:, column(s, h, mine)]
                c = copy(3, s, h, d, block, block)
            out.append(c)
        return out

    started = {}

    def start(stage, s, h):
        started[stage, s, h] = copies(stage, s, h)
        for c in started[stage, s, h]:
            c.start()

    for s in range(SLICES):
        for h in (0, 1):
            cd[2 * s + h].wait()
            t = jnp.dot(hid[...], wd[2 * s + h], preferred_element_type=F32)
            for k in range(side):
                piece = t[:, k * cw : (k + 1) * cw]
                term[s, h, k] = piece
                send[s, h, k] = piece.astype(BF16)
            if s == 0 and h == 0:
                pl.semaphore_wait(barrier, 2 * (side - 1))
            start(0, s, h)

    def advance(stage, s, h):
        for c in started[stage, s, h]:
            c.wait_recv()
        mine, other = pos[h], pos[1 - h]
        if stage == 0:
            total = term[s, h, mine]
            for d in range(side - 1):
                total = total + part[s, h, d].astype(F32)
            psum[s, h] = total
            pout[s, h] = total.astype(BF16)
            start(1, s, h)
        elif stage == 1:
            own = pl.ds(pl.multiple_of(other * quarter, quarter), quarter)
            total = psum[s, h, own, :]
            for d in range(side - 1):
                total = total + p2[s, h, d].astype(F32)
            y[own, column(s, h, mine)] = total.astype(BF16)
            start(2, s, h)
        elif stage == 2:
            start(3, s, h)

    for tick in range(SLICES + 3):
        for s in range(SLICES):
            if 0 <= tick - s < 4:
                for h in (0, 1):
                    advance(tick - s, s, h)
    for group in started.values():
        for c in group:
            c.wait_send()


def solution(mesh):
    side = math.isqrt(mesh.shape["tp"])

    def step(x, w_gate, w_up, w_down):
        rows, depth = x.shape
        units = w_gate.shape[1]
        cw = depth // (2 * SLICES * side)
        blocks = units // BLOCK
        quarter = rows // side
        count = SLICES * 2 * 4 * (side - 1)
        return pl.pallas_call(
            functools.partial(_kernel, side),
            out_shape=jax.ShapeDtypeStruct((rows, depth), BF16),
            in_specs=[pl.BlockSpec(memory_space=pltpu.HBM)] * 4,
            out_specs=pl.BlockSpec(memory_space=pltpu.VMEM),
            scratch_shapes=[
                pltpu.VMEM((rows, depth), BF16),
                pltpu.VMEM((blocks, depth, BLOCK), BF16),
                pltpu.VMEM((blocks, depth, BLOCK), BF16),
                pltpu.VMEM((2 * SLICES, units, side * cw), BF16),
                pltpu.VMEM((rows, units), BF16),
                pltpu.VMEM((SLICES, 2, side, rows, cw), F32),
                pltpu.VMEM((SLICES, 2, side, rows, cw), BF16),
                pltpu.VMEM((SLICES, 2, side - 1, rows, cw), BF16),
                pltpu.VMEM((SLICES, 2, rows, cw), F32),
                pltpu.VMEM((SLICES, 2, rows, cw), BF16),
                pltpu.VMEM((SLICES, 2, side - 1, quarter, cw), BF16),
                pltpu.SemaphoreType.DMA((1 + 2 * blocks + 2 * SLICES,)),
                pltpu.SemaphoreType.DMA((count,)),
                pltpu.SemaphoreType.DMA((count,)),
            ],
            compiler_params=pltpu.CompilerParams(
                collective_id=0, has_side_effects=True, vmem_limit_bytes=44 * 2**20
            ),
            name="mlp_block",
        )(*(pltpu.with_memory_space_constraint(a, pltpu.HBM) for a in (x, w_gate, w_up, w_down)))

    return jax.shard_map(
        step,
        mesh=mesh,
        in_specs=(P("dp", None), P(None, "tp"), P(None, "tp"), P("tp", None)),
        out_specs=P("dp", None),
        check_vma=False,
    )
```

```python
import functools
import math

import jax
import jax.numpy as jnp
from jax import lax
from jax.experimental import pallas as pl
from jax.experimental.pallas import tpu as pltpu
from jax.sharding import PartitionSpec as P

F32, BF16 = jnp.float32, jnp.bfloat16
MESH = pl.DeviceIdType.MESH
SLICES = 3
BLOCK = 256


def _kernel(side, x_hbm, wg_hbm, wu_hbm, wd_hbm, y, xv, wg, wu, wd, hid, term, send, part, psum, pout, p2, local_sem, ssem, rsem):
    me = lax.axis_index("tp")
    pos = (me // side, me % side)
    rows, depth = x_hbm.shape
    units = wg_hbm.shape[1]
    cw = send.shape[-1]
    span = side * cw
    quarter = rows // side

    def peer(axis, d):
        p = list(pos)
        p[axis] = lax.rem(p[axis] + d, side)
        return p[0] * side + p[1]

    barrier = pltpu.get_barrier_semaphore()
    for axis in (0, 1):
        for d in range(1, side):
            pl.semaphore_signal(barrier, inc=1, device_id={"tp": peer(axis, d)}, device_id_type=MESH)

    blocks = units // BLOCK
    cx = pltpu.make_async_copy(x_hbm, xv, local_sem.at[0])
    cx.start()
    cg, cu, cd = [], [], []
    for j in range(blocks):
        cols = pl.ds(j * BLOCK, BLOCK)
        cg.append(pltpu.make_async_copy(wg_hbm.at[:, cols], wg.at[j], local_sem.at[1 + j]))
        cu.append(pltpu.make_async_copy(wu_hbm.at[:, cols], wu.at[j], local_sem.at[1 + blocks + j]))
        cg[j].start()
        cu[j].start()
    for i in range(2 * SLICES):
        cd.append(pltpu.make_async_copy(wd_hbm.at[:, pl.ds(i * span, span)], wd.at[i], local_sem.at[1 + 2 * blocks + i]))
        cd[i].start()

    cx.wait()
    for j in range(blocks):
        cg[j].wait()
        gate = jnp.dot(xv[...], wg[j], preferred_element_type=F32)
        cu[j].wait()
        up = jnp.dot(xv[...], wu[j], preferred_element_type=F32)
        hid[:, j * BLOCK : (j + 1) * BLOCK] = (jax.nn.gelu(gate) * up).astype(BF16)

    def column(s, h, t):
        return pl.ds(pl.multiple_of((2 * s + h) * span + t * cw, cw), cw)

    def copy(stage, s, h, d, src, dst):
        axis = h if stage in (0, 3) else 1 - h
        i = ((s * 2 + h) * 4 + stage) * (side - 1) + d - 1
        return pltpu.make_async_remote_copy(
            src_ref=src,
            dst_ref=dst,
            send_sem=ssem.at[i],
            recv_sem=rsem.at[i],
            device_id={"tp": peer(axis, d)},
            device_id_type=MESH,
        )

    def copies(stage, s, h):
        mine, other = pos[h], pos[1 - h]
        out = []
        for d in range(1, side):
            if stage == 0:
                c = copy(0, s, h, d, send.at[s, h, lax.rem(mine + d, side)], part.at[s, h, d - 1])
            elif stage == 1:
                to = pl.multiple_of(lax.rem(other + d, side) * quarter, quarter)
                c = copy(1, s, h, d, pout.at[s, h, pl.ds(to, quarter)], p2.at[s, h, d - 1])
            elif stage == 2:
                block = y.at[pl.ds(pl.multiple_of(other * quarter, quarter), quarter), column(s, h, mine)]
                c = copy(2, s, h, d, block, block)
            else:
                block = y.at[:, column(s, h, mine)]
                c = copy(3, s, h, d, block, block)
            out.append(c)
        return out

    started = {}

    def start(stage, s, h):
        started[stage, s, h] = copies(stage, s, h)
        for c in started[stage, s, h]:
            c.start()

    for s in range(SLICES):
        for h in (0, 1):
            cd[2 * s + h].wait()
            t = jnp.dot(hid[...], wd[2 * s + h], preferred_element_type=F32)
            for k in range(side):
                piece = t[:, k * cw : (k + 1) * cw]
                term[s, h, k] = piece
                send[s, h, k] = piece.astype(BF16)
            if s == 0 and h == 0:
                pl.semaphore_wait(barrier, 2 * (side - 1))
            start(0, s, h)

    def advance(stage, s, h):
        for c in started[stage, s, h]:
            c.wait_recv()
        mine, other = pos[h], pos[1 - h]
        if stage == 0:
            total = term[s, h, mine]
            for d in range(side - 1):
                total = total + part[s, h, d].astype(F32)
            psum[s, h] = total
            pout[s, h] = total.astype(BF16)
            start(1, s, h)
        elif stage == 1:
            own = pl.ds(pl.multiple_of(other * quarter, quarter), quarter)
            total = psum[s, h, own, :]
            for d in range(side - 1):
                total = total + p2[s, h, d].astype(F32)
            y[own, column(s, h, mine)] = total.astype(BF16)
            start(2, s, h)
        elif stage == 2:
            start(3, s, h)

    for stage in range(4):
        for s in range(SLICES):
            for h in (0, 1):
                advance(stage, s, h)
    for group in started.values():
        for c in group:
            c.wait_send()


def solution(mesh):
    side = math.isqrt(mesh.shape["tp"])

    def step(x, w_gate, w_up, w_down):
        rows, depth = x.shape
        units = w_gate.shape[1]
        cw = depth // (2 * SLICES * side)
        blocks = units // BLOCK
        quarter = rows // side
        count = SLICES * 2 * 4 * (side - 1)
        return pl.pallas_call(
            functools.partial(_kernel, side),
            out_shape=jax.ShapeDtypeStruct((rows, depth), BF16),
            in_specs=[pl.BlockSpec(memory_space=pltpu.HBM)] * 4,
            out_specs=pl.BlockSpec(memory_space=pltpu.VMEM),
            scratch_shapes=[
                pltpu.VMEM((rows, depth), BF16),
                pltpu.VMEM((blocks, depth, BLOCK), BF16),
                pltpu.VMEM((blocks, depth, BLOCK), BF16),
                pltpu.VMEM((2 * SLICES, units, side * cw), BF16),
                pltpu.VMEM((rows, units), BF16),
                pltpu.VMEM((SLICES, 2, side, rows, cw), F32),
                pltpu.VMEM((SLICES, 2, side, rows, cw), BF16),
                pltpu.VMEM((SLICES, 2, side - 1, rows, cw), BF16),
                pltpu.VMEM((SLICES, 2, rows, cw), F32),
                pltpu.VMEM((SLICES, 2, rows, cw), BF16),
                pltpu.VMEM((SLICES, 2, side - 1, quarter, cw), BF16),
                pltpu.SemaphoreType.DMA((1 + 2 * blocks + 2 * SLICES,)),
                pltpu.SemaphoreType.DMA((count,)),
                pltpu.SemaphoreType.DMA((count,)),
            ],
            compiler_params=pltpu.CompilerParams(
                collective_id=0, has_side_effects=True, vmem_limit_bytes=44 * 2**20
            ),
            name="mlp_block",
        )(*(pltpu.with_memory_space_constraint(a, pltpu.HBM) for a in (x, w_gate, w_up, w_down)))

    return jax.shard_map(
        step,
        mesh=mesh,
        in_specs=(P("dp", None), P(None, "tp"), P(None, "tp"), P("tp", None)),
        out_specs=P("dp", None),
        check_vma=False,
    )
```

```python
import contextlib
import functools
import math

import jax
import jax.numpy as jnp
from jax import lax
from jax.experimental import pallas as pl
from jax.experimental.pallas import tpu as pltpu
from jax.sharding import PartitionSpec as P

F32, BF16 = jnp.float32, jnp.bfloat16
MESH = pl.DeviceIdType.MESH
BLOCK = 256
PIECE = 128
PARTS = 2


def scope(name):
    return contextlib.nullcontext()


def _kernel(side, x_hbm, wg_hbm, wu_hbm, wd_hbm, y, xv, wg, wu, wd, hid, acc, send, part, quad, outb, local_sem, xsem, hsem, ssem, rsem):
    dp, tp = lax.axis_index("dp"), lax.axis_index("tp")
    core = lax.rem(dp, 2)
    mate = dp + 1 - 2 * core
    pos = (tp // side, lax.rem(tp, side))
    rows = x_hbm.shape[0]
    blocks = wg.shape[0]
    half_units = blocks * BLOCK
    slices = wd.shape[1]
    span = side * PIECE
    high = rows // PARTS
    order = (2, 1, 3) if side == 4 else tuple(range(1, side))

    def peer(group, axis, d):
        p = list(pos)
        p[axis] = lax.rem(p[axis] + d, side)
        return {"dp": group, "tp": p[0] * side + p[1]}

    def remote(src, dst, send_sem, recv_sem, device):
        c = pltpu.make_async_remote_copy(
            src_ref=src, dst_ref=dst, send_sem=send_sem, recv_sem=recv_sem, device_id=device, device_id_type=MESH
        )
        c.start()

    def wait(ref, sem):
        pltpu.make_async_copy(ref, ref, sem).wait()

    barrier = pltpu.get_barrier_semaphore()
    others = [peer(dp, axis, d) for axis in (0, 1) for d in order] + [peer(mate, 1, d) for d in (0,) + order]
    for device in others:
        pl.semaphore_signal(barrier, inc=1, device_id=device, device_id_type=MESH)

    cx = pltpu.make_async_copy(x_hbm, xv.at[pl.ds(0, rows)], local_sem.at[0])
    cx.start()
    cg, cu, cd = [], [], {}
    for j in range(blocks):
        cols = pl.ds(pl.multiple_of(core * half_units + j * BLOCK, BLOCK), BLOCK)
        cg.append(pltpu.make_async_copy(wg_hbm.at[:, cols], wg.at[j], local_sem.at[1 + j]))
        cu.append(pltpu.make_async_copy(wu_hbm.at[:, cols], wu.at[j], local_sem.at[1 + blocks + j]))
        cg[j].start()
        cu[j].start()
    base = pl.multiple_of(core * slices * span, span)
    for k in (0, 1):
        units = pl.ds(pl.multiple_of((core if k == 0 else 1 - core) * half_units, BLOCK), half_units)
        for s in range(slices):
            cd[k, s] = pltpu.make_async_copy(
                wd_hbm.at[units, pl.ds(pl.multiple_of(base + s * span, span), span)],
                wd.at[k, s],
                local_sem.at[1 + 2 * blocks + k * slices + s],
            )
            cd[k, s].start()

    def hidden(j, first, count):
        at = pl.ds(first * rows, count * rows)
        gate = jnp.dot(xv[at], wg[j], preferred_element_type=F32)
        up = jnp.dot(xv[at], wu[j], preferred_element_type=F32)
        cols = pl.ds(j * BLOCK, BLOCK)
        hid[0, at, cols] = (jax.nn.gelu(gate) * up).astype(BF16)
        for g in range(first, first + count):
            remote(
                hid.at[0, pl.ds(g * rows, rows), cols],
                hid.at[1, pl.ds((1 - g) * rows, rows), cols],
                hsem.at[0],
                hsem.at[1],
                {"dp": mate, "tp": tp},
            )

    def loaded(j):
        with scope(f"gw{j}"):
            cg[j].wait()
            cu[j].wait()

    with scope("xw"):
        cx.wait()
    with scope("barw"):
        pl.semaphore_wait(barrier, len(others))
    remote(xv.at[pl.ds(0, rows)], xv.at[pl.ds(rows, rows)], xsem.at[0], xsem.at[1], {"dp": mate, "tp": tp})
    for j in range(blocks - 1):
        loaded(j)
        hidden(j, 0, 1)
    with scope("xrw"):
        wait(xv.at[pl.ds(rows, rows)], xsem.at[1])
    hidden(0, 1, 1)
    loaded(blocks - 1)
    hidden(blocks - 1, 0, 2)
    for j in range(1, blocks - 1):
        hidden(j, 1, 1)

    def column(s):
        return lambda t: pl.ds(pl.multiple_of(base + s * span + t * PIECE, PIECE), PIECE)

    def start(stage, u, h):
        s, r = u // PARTS, u % PARTS
        mine, other = pos[h], pos[1 - h]
        sem = rsem.at[(stage * slices * PARTS + u) * 2 + h]
        if stage == 0:
            for d in order:
                to = lax.rem(mine + d, side)
                remote(send.at[h, u, to], part.at[h, u, d - 1], ssem.at[0], sem, peer(dp, h, d))
        elif stage == 1:
            for d in order:
                remote(quad.at[h, u, other], quad.at[h, u, other], ssem.at[1], sem, peer(dp, 1 - h, d))
        else:
            block = y.at[pl.ds(r * high, high), column(s)(mine)]
            if h == 0:
                for d in order:
                    remote(block, block, ssem.at[2], sem, peer(dp, h, d))
            else:
                for d in order + (0,):
                    remote(outb.at[u], block, ssem.at[3], sem, peer(mate, h, d))

    for s in range(slices):
        with scope(f"dw0{s}"):
            cd[0, s].wait()
        acc[s] = jnp.dot(hid[0], wd[0, s], preferred_element_type=F32)
    with scope("hrw"):
        wait(hid.at[1], hsem.at[1])
    for s in range(slices):
        with scope(f"dw1{s}"):
            cd[1, s].wait()
        t = acc[s] + jnp.dot(hid[1], wd[1, s], preferred_element_type=F32)
        acc[s] = t
        for h in (0, 1):
            for r in range(PARTS):
                at = h * rows + r * high
                for k in range(side):
                    send[h, s * PARTS + r, k] = t[at : at + high, k * PIECE : (k + 1) * PIECE].astype(BF16)
        with scope(f"snd{s}"):
            for r in range(PARTS):
                for h in (0, 1):
                    start(0, s * PARTS + r, h)

    events = sorted((u + 7 * stage, u, stage) for u in range(slices * PARTS) for stage in range(3))
    for _, u, stage in events:
        s, r = u // PARTS, u % PARTS
        for h in (0, 1):
            mine, other = pos[h], pos[1 - h]
            with scope(f"rw{stage}_{u}{h}"):
                wait(quad.at[h, u] if stage == 2 and h == 1 else part.at[h, u], rsem.at[(stage * slices * PARTS + u) * 2 + h])
            if stage == 0:
                total = acc[s, pl.ds(h * rows + r * high, high), pl.ds(pl.multiple_of(mine * PIECE, PIECE), PIECE)]
                for d in range(side - 1):
                    total = total + part[h, u, d].astype(F32)
                quad[h, u, other] = total.astype(BF16)
                start(1, u, h)
            elif stage == 1:
                total = quad[h, u, 0].astype(F32)
                for k in range(1, side):
                    total = total + quad[h, u, k].astype(F32)
                if h == 0:
                    y[pl.ds(r * high, high), column(s)(mine)] = total.astype(BF16)
                else:
                    outb[u] = total.astype(BF16)
                start(2, u, h)
    with scope("sw"):
        wait(xv.at[pl.ds(0, rows)], xsem.at[0])
        wait(hid.at[0], hsem.at[0])
        wait(part, ssem.at[0])
        wait(part, ssem.at[1])
        wait(part.at[0], ssem.at[2])
        wait(quad.at[1], ssem.at[3])


def solution(mesh):
    side = math.isqrt(mesh.shape["tp"])

    def step(x, w_gate, w_up, w_down):
        rows, depth = x.shape
        half_units = w_gate.shape[1] // 2
        blocks = half_units // BLOCK
        slices = depth // (2 * side * PIECE)
        count = slices * PARTS
        high = rows // PARTS
        return pl.pallas_call(
            functools.partial(_kernel, side),
            out_shape=jax.ShapeDtypeStruct((rows, depth), BF16),
            in_specs=[pl.BlockSpec(memory_space=pltpu.HBM)] * 4,
            out_specs=pl.BlockSpec(memory_space=pltpu.VMEM),
            scratch_shapes=[
                pltpu.VMEM((2 * rows, depth), BF16),
                pltpu.VMEM((blocks, depth, BLOCK), BF16),
                pltpu.VMEM((blocks, depth, BLOCK), BF16),
                pltpu.VMEM((2, slices, half_units, side * PIECE), BF16),
                pltpu.VMEM((2, 2 * rows, half_units), BF16),
                pltpu.VMEM((slices, 2 * rows, side * PIECE), F32),
                pltpu.VMEM((2, count, side, high, PIECE), BF16),
                pltpu.VMEM((2, count, side - 1, high, PIECE), BF16),
                pltpu.VMEM((2, count, side, high, PIECE), BF16),
                pltpu.VMEM((count, high, PIECE), BF16),
                pltpu.SemaphoreType.DMA((1 + 2 * blocks + 2 * slices,)),
                pltpu.SemaphoreType.DMA((2,)),
                pltpu.SemaphoreType.DMA((2,)),
                pltpu.SemaphoreType.DMA((4,)),
                pltpu.SemaphoreType.DMA((3 * count * 2,)),
            ],
            compiler_params=pltpu.CompilerParams(
                collective_id=0, has_side_effects=True, vmem_limit_bytes=40 * 2**20
            ),
            name="mlp_block",
        )(*(pltpu.with_memory_space_constraint(a, pltpu.HBM) for a in (x, w_gate, w_up, w_down)))

    return jax.shard_map(
        step,
        mesh=mesh,
        in_specs=(P("dp", None), P(None, "tp"), P(None, "tp"), P("tp", None)),
        out_specs=P("dp", None),
        check_vma=False,
    )
```

```python
import contextlib
import functools
import math

import jax
import jax.numpy as jnp
from jax import lax
from jax.experimental import pallas as pl
from jax.experimental.pallas import tpu as pltpu
from jax.sharding import PartitionSpec as P

F32, BF16 = jnp.float32, jnp.bfloat16
MESH = pl.DeviceIdType.MESH
BLOCK = 256
PIECE = 128
PARTS = 2


def scope(name):
    return contextlib.nullcontext()


def _kernel(side, x_hbm, wg_hbm, wu_hbm, wd_hbm, y, xv, wg, wu, wd, hid, acc, send, part, quad, outb, local_sem, xsem, hsem, ssem, rsem):
    dp, tp = lax.axis_index("dp"), lax.axis_index("tp")
    core = lax.rem(dp, 2)
    mate = dp + 1 - 2 * core
    pos = (tp // side, lax.rem(tp, side))
    rows = x_hbm.shape[0]
    blocks = wg.shape[0]
    half_units = blocks * BLOCK
    slices = wd.shape[1]
    span = side * PIECE
    high = rows // PARTS
    order = (2, 1, 3) if side == 4 else tuple(range(1, side))

    def peer(group, axis, d):
        p = list(pos)
        p[axis] = lax.rem(p[axis] + d, side)
        return {"dp": group, "tp": p[0] * side + p[1]}

    def remote(src, dst, send_sem, recv_sem, device):
        c = pltpu.make_async_remote_copy(
            src_ref=src, dst_ref=dst, send_sem=send_sem, recv_sem=recv_sem, device_id=device, device_id_type=MESH
        )
        c.start()

    def wait(ref, sem):
        pltpu.make_async_copy(ref, ref, sem).wait()

    barrier = pltpu.get_barrier_semaphore()
    others = [peer(group, axis, d) for group in (dp, mate) for axis in (0, 1) for d in order] + [peer(mate, 0, 0)]
    for device in others:
        pl.semaphore_signal(barrier, inc=1, device_id=device, device_id_type=MESH)

    cx = pltpu.make_async_copy(x_hbm, xv.at[pl.ds(0, rows)], local_sem.at[0])
    cx.start()
    cg, cu, cd = [], [], {}
    for j in range(blocks):
        cols = pl.ds(pl.multiple_of(core * half_units + j * BLOCK, BLOCK), BLOCK)
        cg.append(pltpu.make_async_copy(wg_hbm.at[:, cols], wg.at[j], local_sem.at[1 + j]))
        cu.append(pltpu.make_async_copy(wu_hbm.at[:, cols], wu.at[j], local_sem.at[1 + blocks + j]))
        cg[j].start()
        cu[j].start()
    base = pl.multiple_of(core * slices * span, span)
    for k in (0, 1):
        units = pl.ds(pl.multiple_of((core if k == 0 else 1 - core) * half_units, BLOCK), half_units)
        for s in range(slices):
            cd[k, s] = pltpu.make_async_copy(
                wd_hbm.at[units, pl.ds(pl.multiple_of(base + s * span, span), span)],
                wd.at[k, s],
                local_sem.at[1 + 2 * blocks + k * slices + s],
            )
            cd[k, s].start()

    def hidden(j, g):
        at, cols = pl.ds(g * rows, rows), pl.ds(j * BLOCK, BLOCK)
        gate = jnp.dot(xv[at], wg[j], preferred_element_type=F32)
        up = jnp.dot(xv[at], wu[j], preferred_element_type=F32)
        hid[0, at, cols] = (jax.nn.gelu(gate) * up).astype(BF16)

    def share(j, g):
        remote(
            hid.at[0, pl.ds(g * rows, rows), pl.ds(j * BLOCK, BLOCK)],
            hid.at[1, pl.ds((1 - g) * rows, rows), pl.ds(j * BLOCK, BLOCK)],
            hsem.at[0],
            hsem.at[1 + g],
            {"dp": mate, "tp": tp},
        )

    with scope("xw"):
        cx.wait()
    with scope("barw"):
        pl.semaphore_wait(barrier, len(others))
    remote(xv.at[pl.ds(0, rows)], xv.at[pl.ds(rows, rows)], xsem.at[0], xsem.at[1], {"dp": mate, "tp": tp})
    for j in range(blocks):
        with scope(f"gw{j}"):
            cg[j].wait()
            cu[j].wait()
        hidden(j, 0)
        share(j, 0)
    with scope("xrw"):
        wait(xv.at[pl.ds(rows, rows)], xsem.at[1])
    for j in range(blocks):
        hidden(j, 1)
    for j in range(blocks):
        share(j, 1)

    def column(s):
        return lambda t: pl.ds(pl.multiple_of(base + s * span + t * PIECE, PIECE), PIECE)

    def start(stage, u, h):
        s, r = u // PARTS, u % PARTS
        axis = (u + h) % 2
        mine, other = pos[axis], pos[1 - axis]
        sem = rsem.at[(stage * slices * PARTS + u) * 2 + h]
        if stage == 0:
            for d in order:
                to = lax.rem(mine + d, side)
                remote(send.at[h, u, to], part.at[h, u, d - 1], ssem.at[0], sem, peer(dp, axis, d))
        elif stage == 1:
            for d in order:
                remote(quad.at[h, u, other], quad.at[h, u, other], ssem.at[1], sem, peer(dp, 1 - axis, d))
        else:
            block = y.at[pl.ds(r * high, high), column(s)(mine)]
            if h == 0:
                for d in order:
                    remote(block, block, ssem.at[2], sem, peer(dp, axis, d))
            else:
                for d in order + (0,):
                    remote(outb.at[u], block, ssem.at[3], sem, peer(mate, axis, d))

    for h in (1, 0):
        with scope(f"hrw{h}"):
            wait(hid.at[0, pl.ds(0, rows)], hsem.at[2 - h])
        at = pl.ds(h * rows, rows)
        for s in range(slices):
            if h == 1:
                with scope(f"dw{s}"):
                    cd[0, s].wait()
                    cd[1, s].wait()
            t = jnp.dot(hid[0, at], wd[0, s], preferred_element_type=F32)
            t = t + jnp.dot(hid[1, at], wd[1, s], preferred_element_type=F32)
            acc[s, at] = t
            for r in range(PARTS):
                for k in range(side):
                    piece = t[r * high : (r + 1) * high, k * PIECE : (k + 1) * PIECE]
                    send[h, s * PARTS + r, k] = piece.astype(BF16)
            with scope(f"snd{h}{s}"):
                for r in range(PARTS):
                    start(0, s * PARTS + r, h)

    for stage in range(3):
        for h, u in [(h, u) for h in (1, 0) for u in range(slices * PARTS)]:
            s, r = u // PARTS, u % PARTS
            axis = (u + h) % 2
            mine, other = pos[axis], pos[1 - axis]
            with scope(f"rw{stage}_{u}{h}"):
                wait(quad.at[h, u] if stage == 2 and h == 1 else part.at[h, u], rsem.at[(stage * slices * PARTS + u) * 2 + h])
            if stage == 0:
                total = acc[s, pl.ds(h * rows + r * high, high), pl.ds(pl.multiple_of(mine * PIECE, PIECE), PIECE)]
                for d in range(side - 1):
                    total = total + part[h, u, d].astype(F32)
                quad[h, u, other] = total.astype(BF16)
                start(1, u, h)
            elif stage == 1:
                total = quad[h, u, 0].astype(F32)
                for k in range(1, side):
                    total = total + quad[h, u, k].astype(F32)
                if h == 0:
                    y[pl.ds(r * high, high), column(s)(mine)] = total.astype(BF16)
                else:
                    outb[u] = total.astype(BF16)
                start(2, u, h)
    with scope("sw"):
        wait(xv.at[pl.ds(0, rows)], xsem.at[0])
        wait(hid.at[0], hsem.at[0])
        wait(part, ssem.at[0])
        wait(part, ssem.at[1])
        wait(part.at[0], ssem.at[2])
        wait(quad.at[1], ssem.at[3])


def solution(mesh):
    side = math.isqrt(mesh.shape["tp"])

    def step(x, w_gate, w_up, w_down):
        rows, depth = x.shape
        half_units = w_gate.shape[1] // 2
        blocks = half_units // BLOCK
        slices = depth // (2 * side * PIECE)
        count = slices * PARTS
        high = rows // PARTS
        return pl.pallas_call(
            functools.partial(_kernel, side),
            out_shape=jax.ShapeDtypeStruct((rows, depth), BF16),
            in_specs=[pl.BlockSpec(memory_space=pltpu.HBM)] * 4,
            out_specs=pl.BlockSpec(memory_space=pltpu.VMEM),
            scratch_shapes=[
                pltpu.VMEM((2 * rows, depth), BF16),
                pltpu.VMEM((blocks, depth, BLOCK), BF16),
                pltpu.VMEM((blocks, depth, BLOCK), BF16),
                pltpu.VMEM((2, slices, half_units, side * PIECE), BF16),
                pltpu.VMEM((2, 2 * rows, half_units), BF16),
                pltpu.VMEM((slices, 2 * rows, side * PIECE), F32),
                pltpu.VMEM((2, count, side, high, PIECE), BF16),
                pltpu.VMEM((2, count, side - 1, high, PIECE), BF16),
                pltpu.VMEM((2, count, side, high, PIECE), BF16),
                pltpu.VMEM((count, high, PIECE), BF16),
                pltpu.SemaphoreType.DMA((1 + 2 * blocks + 2 * slices,)),
                pltpu.SemaphoreType.DMA((2,)),
                pltpu.SemaphoreType.DMA((3,)),
                pltpu.SemaphoreType.DMA((4,)),
                pltpu.SemaphoreType.DMA((3 * count * 2,)),
            ],
            compiler_params=pltpu.CompilerParams(
                collective_id=0, has_side_effects=True, vmem_limit_bytes=40 * 2**20
            ),
            name="mlp_block",
        )(*(pltpu.with_memory_space_constraint(a, pltpu.HBM) for a in (x, w_gate, w_up, w_down)))

    return jax.shard_map(
        step,
        mesh=mesh,
        in_specs=(P("dp", None), P(None, "tp"), P(None, "tp"), P("tp", None)),
        out_specs=P("dp", None),
        check_vma=False,
    )
```

```python
import contextlib
import functools
import math

import jax
import jax.numpy as jnp
from jax import lax
from jax.experimental import pallas as pl
from jax.experimental.pallas import tpu as pltpu
from jax.sharding import PartitionSpec as P

F32, BF16 = jnp.float32, jnp.bfloat16
MESH = pl.DeviceIdType.MESH
BLOCK = 256
PIECE = 128
PARTS = 2


def scope(name):
    return contextlib.nullcontext()


def _kernel(side, x_hbm, wg_hbm, wu_hbm, wd_hbm, y, xv, wgu, wd, hid, acc, send, part, quad, outb, local_sem, xsem, hsem, ssem, rsem):
    dp, tp = lax.axis_index("dp"), lax.axis_index("tp")
    core = lax.rem(dp, 2)
    mate = dp + 1 - 2 * core
    pos = (tp // side, lax.rem(tp, side))
    rows, depth = x_hbm.shape
    blocks = wgu.shape[0]
    half_units = blocks * BLOCK
    slices = wd.shape[1]
    span = side * PIECE
    high = rows // PARTS
    order = (2, 1, 3) if side == 4 else tuple(range(1, side))

    def peer(group, axis, d):
        p = list(pos)
        p[axis] = lax.rem(p[axis] + d, side)
        return {"dp": group, "tp": p[0] * side + p[1]}

    def remote(src, dst, send_sem, recv_sem, device):
        c = pltpu.make_async_remote_copy(
            src_ref=src, dst_ref=dst, send_sem=send_sem, recv_sem=recv_sem, device_id=device, device_id_type=MESH
        )
        c.start()

    def wait(ref, sem):
        pltpu.make_async_copy(ref, ref, sem).wait()

    barrier = pltpu.get_barrier_semaphore()
    others = [peer(group, axis, d) for group in (dp, mate) for axis in (0, 1) for d in order] + [peer(mate, 0, 0)]
    for device in others:
        pl.semaphore_signal(barrier, inc=1, device_id=device, device_id_type=MESH)

    cx = pltpu.make_async_copy(x_hbm, xv.at[pl.ds(0, rows)], local_sem.at[0])
    cx.start()
    for j in range(blocks):
        cols = pl.ds(pl.multiple_of(core * half_units + j * BLOCK, BLOCK), BLOCK)
        for k, w in enumerate((wg_hbm, wu_hbm)):
            load = pltpu.make_async_copy(w.at[:, cols], wgu.at[j, :, pl.ds(k * BLOCK, BLOCK)], local_sem.at[1 + j])
            load.start()
    base = pl.multiple_of(core * slices * span, span)
    for s in range(slices):
        for k in (0, 1):
            units = pl.ds(pl.multiple_of((core if k == 0 else 1 - core) * half_units, BLOCK), half_units)
            cols = pl.ds(pl.multiple_of(base + s * span, span), span)
            load = pltpu.make_async_copy(wd_hbm.at[units, cols], wd.at[k, s], local_sem.at[1 + blocks + s])
            load.start()

    def hidden(j, g):
        at, cols = pl.ds(g * rows, rows), pl.ds(j * BLOCK, BLOCK)
        both = jnp.dot(xv[at], wgu[j], preferred_element_type=F32)
        hid[0, at, cols] = (jax.nn.gelu(both[:, :BLOCK]) * both[:, BLOCK:]).astype(BF16)

    def share(j, g):
        remote(
            hid.at[0, pl.ds(g * rows, rows), pl.ds(j * BLOCK, BLOCK)],
            hid.at[1, pl.ds((1 - g) * rows, rows), pl.ds(j * BLOCK, BLOCK)],
            ssem,
            hsem.at[g],
            {"dp": mate, "tp": tp},
        )

    with scope("xw"):
        cx.wait()
    with scope("barw"):
        pl.semaphore_wait(barrier, len(others))
    remote(xv.at[pl.ds(0, rows)], xv.at[pl.ds(rows, rows)], ssem, xsem, {"dp": mate, "tp": tp})
    for j in range(blocks):
        with scope(f"gw{j}"):
            wait(wgu.at[j], local_sem.at[1 + j])
        hidden(j, 0)
        share(j, 0)
    with scope("xrw"):
        wait(xv.at[pl.ds(rows, rows)], xsem)
    for j in range(blocks):
        hidden(j, 1)
    for j in range(blocks):
        share(j, 1)

    def column(s):
        return lambda t: pl.ds(pl.multiple_of(base + s * span + t * PIECE, PIECE), PIECE)

    def start(stage, u, h):
        s, r = u // PARTS, u % PARTS
        axis = (u + h) % 2
        mine, other = pos[axis], pos[1 - axis]
        sem = rsem.at[min(stage * slices * PARTS + u, 2 * slices * PARTS) * 2 + (h if stage < 2 else 0)]
        if stage == 0:
            for d in order:
                to = lax.rem(mine + d, side)
                remote(send.at[h, u, to], part.at[h, u, d - 1], ssem, sem, peer(dp, axis, d))
        elif stage == 1:
            for d in order:
                remote(quad.at[h, u, other], quad.at[h, u, other], ssem, sem, peer(dp, 1 - axis, d))
        else:
            block = y.at[pl.ds(r * high, high), column(s)(mine)]
            if h == 0:
                for d in order:
                    remote(block, block, ssem, sem, peer(dp, axis, d))
            else:
                for d in order + (0,):
                    remote(outb.at[u], block, ssem, sem, peer(mate, axis, d))

    for h in (1, 0):
        with scope(f"hrw{h}"):
            wait(hid.at[0, pl.ds(0, rows)], hsem.at[1 - h])
        at = pl.ds(h * rows, rows)
        for s in range(slices):
            if h == 1:
                with scope(f"dw{s}"):
                    wait(wd.at[:, s], local_sem.at[1 + blocks + s])
            t = jnp.dot(hid[0, at], wd[0, s], preferred_element_type=F32)
            t = t + jnp.dot(hid[1, at], wd[1, s], preferred_element_type=F32)
            acc[s, at] = t
            for r in range(PARTS):
                for k in range(side):
                    piece = t[r * high : (r + 1) * high, k * PIECE : (k + 1) * PIECE]
                    send[h, s * PARTS + r, k] = piece.astype(BF16)
            with scope(f"snd{h}{s}"):
                for r in range(PARTS):
                    start(0, s * PARTS + r, h)

    for stage in range(2):
        for h, u in [(h, u) for h in (1, 0) for u in range(slices * PARTS)]:
            s, r = u // PARTS, u % PARTS
            axis = (u + h) % 2
            mine, other = pos[axis], pos[1 - axis]
            with scope(f"rw{stage}_{u}{h}"):
                wait(part.at[h, u], rsem.at[(stage * slices * PARTS + u) * 2 + h])
            if stage == 0:
                total = acc[s, pl.ds(h * rows + r * high, high), pl.ds(pl.multiple_of(mine * PIECE, PIECE), PIECE)]
                for d in range(side - 1):
                    total = total + part[h, u, d].astype(F32)
                quad[h, u, other] = total.astype(BF16)
                start(1, u, h)
            else:
                total = quad[h, u, 0].astype(F32)
                for k in range(1, side):
                    total = total + quad[h, u, k].astype(F32)
                if h == 0:
                    y[pl.ds(r * high, high), column(s)(mine)] = total.astype(BF16)
                else:
                    outb[u] = total.astype(BF16)
                start(2, u, h)
    pieces = slices * PARTS * high * PIECE
    taken = (2 * side - 1) * pieces
    with scope("ew"):
        wait(wd.at[:, :, pl.ds(0, taken // (2 * slices * span))], rsem.at[4 * slices * PARTS])
    given = 2 * rows * half_units + rows * depth + (4 * (side - 1) + 2 * side - 1) * pieces
    with scope("sw"):
        wait(wd.at[:, :, pl.ds(0, given // (2 * slices * span))], ssem)


def solution(mesh):
    side = math.isqrt(mesh.shape["tp"])

    def step(x, w_gate, w_up, w_down):
        rows, depth = x.shape
        half_units = w_gate.shape[1] // 2
        blocks = half_units // BLOCK
        slices = depth // (2 * side * PIECE)
        count = slices * PARTS
        high = rows // PARTS
        return pl.pallas_call(
            functools.partial(_kernel, side),
            out_shape=jax.ShapeDtypeStruct((rows, depth), BF16),
            in_specs=[pl.BlockSpec(memory_space=pltpu.HBM)] * 4,
            out_specs=pl.BlockSpec(memory_space=pltpu.VMEM),
            scratch_shapes=[
                pltpu.VMEM((2 * rows, depth), BF16),
                pltpu.VMEM((blocks, depth, 2 * BLOCK), BF16),
                pltpu.VMEM((2, slices, half_units, side * PIECE), BF16),
                pltpu.VMEM((2, 2 * rows, half_units), BF16),
                pltpu.VMEM((slices, 2 * rows, side * PIECE), F32),
                pltpu.VMEM((2, count, side, high, PIECE), BF16),
                pltpu.VMEM((2, count, side - 1, high, PIECE), BF16),
                pltpu.VMEM((2, count, side, high, PIECE), BF16),
                pltpu.VMEM((count, high, PIECE), BF16),
                pltpu.SemaphoreType.DMA((1 + blocks + slices,)),
                pltpu.SemaphoreType.DMA,
                pltpu.SemaphoreType.DMA((2,)),
                pltpu.SemaphoreType.DMA,
                pltpu.SemaphoreType.DMA((4 * count + 1,)),
            ],
            compiler_params=pltpu.CompilerParams(
                collective_id=0, has_side_effects=True, vmem_limit_bytes=40 * 2**20
            ),
            name="mlp_block",
        )(*(pltpu.with_memory_space_constraint(a, pltpu.HBM) for a in (x, w_gate, w_up, w_down)))

    return jax.shard_map(
        step,
        mesh=mesh,
        in_specs=(P("dp", None), P(None, "tp"), P(None, "tp"), P("tp", None)),
        out_specs=P("dp", None),
        check_vma=False,
    )
```

```python
import contextlib
import functools
import math

import jax
import jax.numpy as jnp
from jax import lax
from jax.experimental import pallas as pl
from jax.experimental.pallas import tpu as pltpu
from jax.sharding import PartitionSpec as P

F32, BF16 = jnp.float32, jnp.bfloat16
MESH = pl.DeviceIdType.MESH
BLOCK = 256
PIECE = 128
PARTS = 2


def scope(name):
    return contextlib.nullcontext()


def _kernel(side, x_hbm, wg_hbm, wu_hbm, wd_hbm, y, xv, wgu, first, wd, hid, acc, send, part, quad, outb, local_sem, xsem, hsem, ssem, rsem):
    dp, tp = lax.axis_index("dp"), lax.axis_index("tp")
    core = lax.rem(dp, 2)
    mate = dp + 1 - 2 * core
    pos = (tp // side, lax.rem(tp, side))
    rows, depth = x_hbm.shape
    blocks = wgu.shape[0]
    half_units = blocks * BLOCK
    slices = wd.shape[1]
    span = side * PIECE
    high = rows // PARTS
    order = (2, 1, 3) if side == 4 else tuple(range(1, side))

    def peer(group, axis, d):
        p = list(pos)
        p[axis] = lax.rem(p[axis] + d, side)
        return {"dp": group, "tp": p[0] * side + p[1]}

    def remote(src, dst, send_sem, recv_sem, device):
        c = pltpu.make_async_remote_copy(
            src_ref=src, dst_ref=dst, send_sem=send_sem, recv_sem=recv_sem, device_id=device, device_id_type=MESH
        )
        c.start()

    def wait(ref, sem):
        pltpu.make_async_copy(ref, ref, sem).wait()

    barrier = pltpu.get_barrier_semaphore()
    others = [peer(group, axis, d) for group in (dp, mate) for axis in (0, 1) for d in order] + [peer(mate, 0, 0)]
    for device in others:
        pl.semaphore_signal(barrier, inc=1, device_id=device, device_id_type=MESH)

    cx = pltpu.make_async_copy(x_hbm, xv.at[pl.ds(0, rows)], local_sem.at[0])
    cx.start()
    deep = (pl.ds(0, depth // 2), pl.ds(depth // 2, depth // 2))
    loads = [(j, pl.ds(0, depth)) for j in range(blocks - 1)] + [(blocks - 1, deep[0]), (blocks - 1, deep[1])]
    for n, (j, at) in enumerate(loads):
        cols = pl.ds(pl.multiple_of(core * half_units + j * BLOCK, BLOCK), BLOCK)
        for k, w in enumerate((wg_hbm, wu_hbm)):
            load = pltpu.make_async_copy(w.at[at, cols], wgu.at[j, at, pl.ds(k * BLOCK, BLOCK)], local_sem.at[1 + n])
            load.start()
    base = pl.multiple_of(core * slices * span, span)
    for s in range(slices):
        for k in (0, 1):
            units = pl.ds(pl.multiple_of((core if k == 0 else 1 - core) * half_units, BLOCK), half_units)
            cols = pl.ds(pl.multiple_of(base + s * span, span), span)
            load = pltpu.make_async_copy(wd_hbm.at[units, cols], wd.at[k, s], local_sem.at[2 + blocks + s])
            load.start()

    def finish(j, g, both):
        hidden = jax.nn.gelu(both[:, :BLOCK]) * both[:, BLOCK:]
        hid[0, pl.ds(g * rows, rows), pl.ds(j * BLOCK, BLOCK)] = hidden.astype(BF16)

    def product(j, g, at):
        return jnp.dot(xv[pl.ds(g * rows, rows), at], wgu[j, at], preferred_element_type=F32)

    def loaded(n):
        j, at = loads[n]
        with scope(f"gw{n}"):
            wait(wgu.at[j, at], local_sem.at[1 + n])

    def share(j, g):
        remote(
            hid.at[0, pl.ds(g * rows, rows), pl.ds(j * BLOCK, BLOCK)],
            hid.at[1, pl.ds((1 - g) * rows, rows), pl.ds(j * BLOCK, BLOCK)],
            ssem,
            hsem.at[g],
            {"dp": mate, "tp": tp},
        )

    whole = pl.ds(0, depth)
    with scope("xw"):
        cx.wait()
    with scope("barw"):
        pl.semaphore_wait(barrier, len(others))
    mine, theirs = pl.ds(0, rows), pl.ds(rows, rows)
    for k in (0, 1):
        remote(xv.at[mine, deep[k]], xv.at[theirs, deep[k]], ssem, xsem.at[k], {"dp": mate, "tp": tp})
    for j in range(blocks - 1):
        loaded(j)
        finish(j, 0, product(j, 0, whole))
        share(j, 0)
    loaded(blocks - 1)
    first[...] = product(blocks - 1, 0, deep[0])
    loaded(blocks)
    finish(blocks - 1, 0, first[...] + product(blocks - 1, 0, deep[1]))
    share(blocks - 1, 0)
    with scope("xrw0"):
        wait(xv.at[theirs, deep[0]], xsem.at[0])
    first[...] = product(0, 1, deep[0])
    with scope("xrw1"):
        wait(xv.at[theirs, deep[1]], xsem.at[1])
    finish(0, 1, first[...] + product(0, 1, deep[1]))
    for j in range(1, blocks):
        finish(j, 1, product(j, 1, whole))
    for j in range(blocks):
        share(j, 1)

    def column(s):
        return lambda t: pl.ds(pl.multiple_of(base + s * span + t * PIECE, PIECE), PIECE)

    def start(stage, u, h):
        s, r = u // PARTS, u % PARTS
        axis = (u + h) % 2
        mine, other = pos[axis], pos[1 - axis]
        sem = rsem.at[min(stage * slices * PARTS + u, 2 * slices * PARTS) * 2 + (h if stage < 2 else 0)]
        if stage == 0:
            for d in order:
                to = lax.rem(mine + d, side)
                remote(send.at[h, u, to], part.at[h, u, d - 1], ssem, sem, peer(dp, axis, d))
        elif stage == 1:
            for d in order:
                remote(quad.at[h, u, other], quad.at[h, u, other], ssem, sem, peer(dp, 1 - axis, d))
        else:
            block = y.at[pl.ds(r * high, high), column(s)(mine)]
            if h == 0:
                for d in order:
                    remote(block, block, ssem, sem, peer(dp, axis, d))
            else:
                for d in order + (0,):
                    remote(outb.at[u], block, ssem, sem, peer(mate, axis, d))

    for h in (1, 0):
        with scope(f"hrw{h}"):
            wait(hid.at[0, pl.ds(0, rows)], hsem.at[1 - h])
        at = pl.ds(h * rows, rows)
        for s in range(slices):
            if h == 1:
                with scope(f"dw{s}"):
                    wait(wd.at[:, s], local_sem.at[2 + blocks + s])
            t = jnp.dot(hid[0, at], wd[0, s], preferred_element_type=F32)
            t = t + jnp.dot(hid[1, at], wd[1, s], preferred_element_type=F32)
            acc[s, at] = t
            for r in range(PARTS):
                for k in range(side):
                    piece = t[r * high : (r + 1) * high, k * PIECE : (k + 1) * PIECE]
                    send[h, s * PARTS + r, k] = piece.astype(BF16)
            with scope(f"snd{h}{s}"):
                for r in range(PARTS):
                    start(0, s * PARTS + r, h)

    for stage in range(2):
        for h, u in [(h, u) for h in (1, 0) for u in range(slices * PARTS)]:
            s, r = u // PARTS, u % PARTS
            axis = (u + h) % 2
            mine, other = pos[axis], pos[1 - axis]
            with scope(f"rw{stage}_{u}{h}"):
                wait(part.at[h, u], rsem.at[(stage * slices * PARTS + u) * 2 + h])
            if stage == 0:
                total = acc[s, pl.ds(h * rows + r * high, high), pl.ds(pl.multiple_of(mine * PIECE, PIECE), PIECE)]
                for d in range(side - 1):
                    total = total + part[h, u, d].astype(F32)
                quad[h, u, other] = total.astype(BF16)
                start(1, u, h)
            else:
                total = quad[h, u, 0].astype(F32)
                for k in range(1, side):
                    total = total + quad[h, u, k].astype(F32)
                if h == 0:
                    y[pl.ds(r * high, high), column(s)(mine)] = total.astype(BF16)
                else:
                    outb[u] = total.astype(BF16)
                start(2, u, h)
    pieces = slices * PARTS * high * PIECE
    taken = (2 * side - 1) * pieces
    with scope("ew"):
        wait(wd.at[:, :, pl.ds(0, taken // (2 * slices * span))], rsem.at[4 * slices * PARTS])
    given = 2 * rows * half_units + rows * depth + (4 * (side - 1) + 2 * side - 1) * pieces
    with scope("sw"):
        wait(wd.at[:, :, pl.ds(0, given // (2 * slices * span))], ssem)


def solution(mesh):
    side = math.isqrt(mesh.shape["tp"])

    def step(x, w_gate, w_up, w_down):
        rows, depth = x.shape
        half_units = w_gate.shape[1] // 2
        blocks = half_units // BLOCK
        slices = depth // (2 * side * PIECE)
        count = slices * PARTS
        high = rows // PARTS
        return pl.pallas_call(
            functools.partial(_kernel, side),
            out_shape=jax.ShapeDtypeStruct((rows, depth), BF16),
            in_specs=[pl.BlockSpec(memory_space=pltpu.HBM)] * 4,
            out_specs=pl.BlockSpec(memory_space=pltpu.VMEM),
            scratch_shapes=[
                pltpu.VMEM((2 * rows, depth), BF16),
                pltpu.VMEM((blocks, depth, 2 * BLOCK), BF16),
                pltpu.VMEM((rows, 2 * BLOCK), F32),
                pltpu.VMEM((2, slices, half_units, side * PIECE), BF16),
                pltpu.VMEM((2, 2 * rows, half_units), BF16),
                pltpu.VMEM((slices, 2 * rows, side * PIECE), F32),
                pltpu.VMEM((2, count, side, high, PIECE), BF16),
                pltpu.VMEM((2, count, side - 1, high, PIECE), BF16),
                pltpu.VMEM((2, count, side, high, PIECE), BF16),
                pltpu.VMEM((count, high, PIECE), BF16),
                pltpu.SemaphoreType.DMA((2 + blocks + slices,)),
                pltpu.SemaphoreType.DMA((2,)),
                pltpu.SemaphoreType.DMA((2,)),
                pltpu.SemaphoreType.DMA,
                pltpu.SemaphoreType.DMA((4 * count + 1,)),
            ],
            compiler_params=pltpu.CompilerParams(
                collective_id=0, has_side_effects=True, vmem_limit_bytes=40 * 2**20
            ),
            name="mlp_block",
        )(*(pltpu.with_memory_space_constraint(a, pltpu.HBM) for a in (x, w_gate, w_up, w_down)))

    return jax.shard_map(
        step,
        mesh=mesh,
        in_specs=(P("dp", None), P(None, "tp"), P(None, "tp"), P("tp", None)),
        out_specs=P("dp", None),
        check_vma=False,
    )
```

```python
import contextlib
import functools
import math

import jax
import jax.numpy as jnp
from jax import lax
from jax.experimental import pallas as pl
from jax.experimental.pallas import tpu as pltpu
from jax.sharding import PartitionSpec as P

F32, BF16 = jnp.float32, jnp.bfloat16
MESH = pl.DeviceIdType.MESH
BLOCK = 256
PIECE = 128
PARTS = 2


def scope(name):
    return contextlib.nullcontext()


def _kernel(side, x_hbm, wg_hbm, wu_hbm, wd_hbm, y, xv, wgu, first, wd, hid, acc, send, part, quad, outb, local_sem, xsem, hsem, ssem, rsem):
    dp, tp = lax.axis_index("dp"), lax.axis_index("tp")
    core = lax.rem(dp, 2)
    mate = dp + 1 - 2 * core
    pos = (tp // side, lax.rem(tp, side))
    rows, depth = x_hbm.shape
    blocks = wgu.shape[0]
    half_units = blocks * BLOCK
    slices = wd.shape[1]
    span = side * PIECE
    high = rows // PARTS
    order = (2, 1, 3) if side == 4 else tuple(range(1, side))

    def peer(group, axis, d):
        p = list(pos)
        p[axis] = lax.rem(p[axis] + d, side)
        return {"dp": group, "tp": p[0] * side + p[1]}

    def remote(src, dst, send_sem, recv_sem, device):
        c = pltpu.make_async_remote_copy(
            src_ref=src, dst_ref=dst, send_sem=send_sem, recv_sem=recv_sem, device_id=device, device_id_type=MESH
        )
        c.start()

    def wait(ref, sem):
        pltpu.make_async_copy(ref, ref, sem).wait()

    barrier = pltpu.get_barrier_semaphore()
    others = [peer(group, axis, d) for group in (dp, mate) for axis in (0, 1) for d in order] + [peer(mate, 0, 0)]
    for device in others:
        pl.semaphore_signal(barrier, inc=1, device_id=device, device_id_type=MESH)

    cx = pltpu.make_async_copy(x_hbm, xv.at[pl.ds(0, rows)], local_sem.at[0])
    cx.start()
    deep = (pl.ds(0, depth // 2), pl.ds(depth // 2, depth // 2))
    loads = [(j, pl.ds(0, depth)) for j in range(blocks - 1)] + [(blocks - 1, deep[0]), (blocks - 1, deep[1])]
    for n, (j, at) in enumerate(loads):
        cols = pl.ds(pl.multiple_of(core * half_units + j * BLOCK, BLOCK), BLOCK)
        for k, w in enumerate((wg_hbm, wu_hbm)):
            load = pltpu.make_async_copy(w.at[at, cols], wgu.at[j, at, pl.ds(k * BLOCK, BLOCK)], local_sem.at[1 + n])
            load.start()
    base = pl.multiple_of(core * slices * span, span)
    for s in range(slices):
        for k in (0, 1):
            units = pl.ds(pl.multiple_of((core if k == 0 else 1 - core) * half_units, BLOCK), half_units)
            cols = pl.ds(pl.multiple_of(base + s * span, span), span)
            load = pltpu.make_async_copy(wd_hbm.at[units, cols], wd.at[k, s], local_sem.at[2 + blocks + s])
            load.start()

    def finish(j, g, both):
        hidden = jax.nn.gelu(both[:, :BLOCK]) * both[:, BLOCK:]
        hid[0, pl.ds(g * rows, rows), pl.ds(j * BLOCK, BLOCK)] = hidden.astype(BF16)

    def product(j, g, at):
        return jnp.dot(xv[pl.ds(g * rows, rows), at], wgu[j, at], preferred_element_type=F32)

    def loaded(n):
        j, at = loads[n]
        with scope(f"gw{n}"):
            wait(wgu.at[j, at], local_sem.at[1 + n])

    def share(j, g, n=1):
        remote(
            hid.at[0, pl.ds(g * rows, rows), pl.ds(j * BLOCK, n * BLOCK)],
            hid.at[1, pl.ds((1 - g) * rows, rows), pl.ds(j * BLOCK, n * BLOCK)],
            ssem,
            hsem.at[g],
            {"dp": mate, "tp": tp},
        )

    whole = pl.ds(0, depth)
    with scope("xw"):
        cx.wait()
    with scope("barw"):
        pl.semaphore_wait(barrier, len(others))
    mine, theirs = pl.ds(0, rows), pl.ds(rows, rows)
    for k in (0, 1):
        remote(xv.at[mine, deep[k]], xv.at[theirs, deep[k]], ssem, xsem.at[k], {"dp": mate, "tp": tp})
    for j in range(blocks - 1):
        loaded(j)
        finish(j, 0, product(j, 0, whole))
        share(j, 0)
    loaded(blocks - 1)
    first[...] = product(blocks - 1, 0, deep[0])
    loaded(blocks)
    finish(blocks - 1, 0, first[...] + product(blocks - 1, 0, deep[1]))
    share(blocks - 1, 0)
    with scope("xrw0"):
        wait(xv.at[theirs, deep[0]], xsem.at[0])
    first[...] = product(0, 1, deep[0])
    with scope("xrw1"):
        wait(xv.at[theirs, deep[1]], xsem.at[1])
    finish(0, 1, first[...] + product(0, 1, deep[1]))
    for j in range(1, blocks):
        finish(j, 1, product(j, 1, whole))
    share(0, 1, blocks)

    def column(s):
        return lambda t: pl.ds(pl.multiple_of(base + s * span + t * PIECE, PIECE), PIECE)

    def start(stage, u, h):
        s, r = u // PARTS, u % PARTS
        axis = (u + h) % 2
        mine, other = pos[axis], pos[1 - axis]
        sem = rsem.at[min(stage * slices * PARTS + u, 2 * slices * PARTS) * 2 + (h if stage < 2 else 0)]
        if stage == 0:
            for d in order:
                to = lax.rem(mine + d, side)
                remote(send.at[h, u, to], part.at[h, u, d - 1], ssem, sem, peer(dp, axis, d))
        elif stage == 1:
            for d in order:
                remote(quad.at[h, u, other], quad.at[h, u, other], ssem, sem, peer(dp, 1 - axis, d))
        else:
            block = y.at[pl.ds(r * high, high), column(s)(mine)]
            if h == 0:
                for d in order:
                    remote(block, block, ssem, sem, peer(dp, axis, d))
            else:
                for d in order + (0,):
                    remote(outb.at[u], block, ssem, sem, peer(mate, axis, d))

    for h in (1, 0):
        with scope(f"hrw{h}"):
            wait(hid.at[0, pl.ds(0, rows)], hsem.at[1 - h])
        at = pl.ds(h * rows, rows)
        for s in range(slices):
            if h == 1:
                with scope(f"dw{s}"):
                    wait(wd.at[:, s], local_sem.at[2 + blocks + s])
            t = jnp.dot(hid[0, at], wd[0, s], preferred_element_type=F32)
            t = t + jnp.dot(hid[1, at], wd[1, s], preferred_element_type=F32)
            for r in range(PARTS):
                for k in range(side):
                    piece = t[r * high : (r + 1) * high, k * PIECE : (k + 1) * PIECE]
                    send[h, s * PARTS + r, k] = piece.astype(BF16)
                with scope(f"snd{h}{s}{r}"):
                    start(0, s * PARTS + r, h)
            acc[s, at] = t

    for stage in range(2):
        for h, u in [(h, u) for h in (1, 0) for u in range(slices * PARTS)]:
            s, r = u // PARTS, u % PARTS
            axis = (u + h) % 2
            mine, other = pos[axis], pos[1 - axis]
            with scope(f"rw{stage}_{u}{h}"):
                wait(part.at[h, u], rsem.at[(stage * slices * PARTS + u) * 2 + h])
            if stage == 0:
                total = acc[s, pl.ds(h * rows + r * high, high), pl.ds(pl.multiple_of(mine * PIECE, PIECE), PIECE)]
                for d in range(side - 1):
                    total = total + part[h, u, d].astype(F32)
                quad[h, u, other] = total.astype(BF16)
                start(1, u, h)
            else:
                total = quad[h, u, 0].astype(F32)
                for k in range(1, side):
                    total = total + quad[h, u, k].astype(F32)
                if h == 0:
                    y[pl.ds(r * high, high), column(s)(mine)] = total.astype(BF16)
                else:
                    outb[u] = total.astype(BF16)
                start(2, u, h)
    pieces = slices * PARTS * high * PIECE
    taken = (2 * side - 1) * pieces
    with scope("ew"):
        wait(wd.at[:, :, pl.ds(0, taken // (2 * slices * span))], rsem.at[4 * slices * PARTS])
    given = 2 * rows * half_units + rows * depth + (4 * (side - 1) + 2 * side - 1) * pieces
    with scope("sw"):
        wait(wd.at[:, :, pl.ds(0, given // (2 * slices * span))], ssem)


def solution(mesh):
    side = math.isqrt(mesh.shape["tp"])

    def step(x, w_gate, w_up, w_down):
        rows, depth = x.shape
        half_units = w_gate.shape[1] // 2
        blocks = half_units // BLOCK
        slices = depth // (2 * side * PIECE)
        count = slices * PARTS
        high = rows // PARTS
        return pl.pallas_call(
            functools.partial(_kernel, side),
            out_shape=jax.ShapeDtypeStruct((rows, depth), BF16),
            in_specs=[pl.BlockSpec(memory_space=pltpu.HBM)] * 4,
            out_specs=pl.BlockSpec(memory_space=pltpu.VMEM),
            scratch_shapes=[
                pltpu.VMEM((2 * rows, depth), BF16),
                pltpu.VMEM((blocks, depth, 2 * BLOCK), BF16),
                pltpu.VMEM((rows, 2 * BLOCK), F32),
                pltpu.VMEM((2, slices, half_units, side * PIECE), BF16),
                pltpu.VMEM((2, 2 * rows, half_units), BF16),
                pltpu.VMEM((slices, 2 * rows, side * PIECE), F32),
                pltpu.VMEM((2, count, side, high, PIECE), BF16),
                pltpu.VMEM((2, count, side - 1, high, PIECE), BF16),
                pltpu.VMEM((2, count, side, high, PIECE), BF16),
                pltpu.VMEM((count, high, PIECE), BF16),
                pltpu.SemaphoreType.DMA((2 + blocks + slices,)),
                pltpu.SemaphoreType.DMA((2,)),
                pltpu.SemaphoreType.DMA((2,)),
                pltpu.SemaphoreType.DMA,
                pltpu.SemaphoreType.DMA((4 * count + 1,)),
            ],
            compiler_params=pltpu.CompilerParams(
                collective_id=0, has_side_effects=True, vmem_limit_bytes=40 * 2**20
            ),
            name="mlp_block",
        )(*(pltpu.with_memory_space_constraint(a, pltpu.HBM) for a in (x, w_gate, w_up, w_down)))

    return jax.shard_map(
        step,
        mesh=mesh,
        in_specs=(P("dp", None), P(None, "tp"), P(None, "tp"), P("tp", None)),
        out_specs=P("dp", None),
        check_vma=False,
    )
```

```python
import contextlib
import functools
import math

import jax
import jax.numpy as jnp
from jax import lax
from jax.experimental import pallas as pl
from jax.experimental.pallas import tpu as pltpu
from jax.sharding import PartitionSpec as P

F32, BF16 = jnp.float32, jnp.bfloat16
MESH = pl.DeviceIdType.MESH
BLOCK = 256
PIECE = 128
PARTS = 2


def scope(name):
    return contextlib.nullcontext()


def _kernel(side, x_hbm, wg_hbm, wu_hbm, wd_hbm, y, xv, wgu, first, wd, hid, acc, send, part, quad, outb, local_sem, xsem, hsem, ssem, rsem):
    dp, tp = lax.axis_index("dp"), lax.axis_index("tp")
    core = lax.rem(dp, 2)
    mate = dp + 1 - 2 * core
    pos = (tp // side, lax.rem(tp, side))
    rows, depth = x_hbm.shape
    blocks = wgu.shape[0]
    half_units = blocks * BLOCK
    slices = wd.shape[1]
    span = side * PIECE
    high = rows // PARTS
    order = (2, 1, 3) if side == 4 else tuple(range(1, side))

    def peer(group, axis, d):
        p = list(pos)
        p[axis] = lax.rem(p[axis] + d, side)
        return {"dp": group, "tp": p[0] * side + p[1]}

    def remote(src, dst, send_sem, recv_sem, device):
        c = pltpu.make_async_remote_copy(
            src_ref=src, dst_ref=dst, send_sem=send_sem, recv_sem=recv_sem, device_id=device, device_id_type=MESH
        )
        c.start()

    def wait(ref, sem):
        pltpu.make_async_copy(ref, ref, sem).wait()

    barrier = pltpu.get_barrier_semaphore()
    others = [peer(mate, 0, 0)] + [peer(group, axis, d) for d in order for group in (mate, dp) for axis in (0, 1)]
    for device in others:
        pl.semaphore_signal(barrier, inc=1, device_id=device, device_id_type=MESH)

    cx = pltpu.make_async_copy(x_hbm, xv.at[pl.ds(0, rows)], local_sem.at[0])
    cx.start()
    deep = (pl.ds(0, depth // 2), pl.ds(depth // 2, depth // 2))
    cut = depth * 7 // 12
    late = (pl.ds(0, cut), pl.ds(cut, depth - cut))
    loads = [(j, pl.ds(0, depth)) for j in range(blocks - 1)] + [(blocks - 1, late[0]), (blocks - 1, late[1])]
    for n, (j, at) in enumerate(loads):
        cols = pl.ds(pl.multiple_of(core * half_units + j * BLOCK, BLOCK), BLOCK)
        for k, w in enumerate((wg_hbm, wu_hbm)):
            load = pltpu.make_async_copy(w.at[at, cols], wgu.at[j, at, pl.ds(k * BLOCK, BLOCK)], local_sem.at[1 + n])
            load.start()
    base = pl.multiple_of(core * slices * span, span)
    for s in range(slices):
        for k in (0, 1):
            units = pl.ds(pl.multiple_of((core if k == 0 else 1 - core) * half_units, BLOCK), half_units)
            cols = pl.ds(pl.multiple_of(base + s * span, span), span)
            load = pltpu.make_async_copy(wd_hbm.at[units, cols], wd.at[k, s], local_sem.at[2 + blocks + s])
            load.start()

    def finish(j, g, both):
        hidden = jax.nn.gelu(both[:, :BLOCK]) * both[:, BLOCK:]
        hid[0, pl.ds(g * rows, rows), pl.ds(j * BLOCK, BLOCK)] = hidden.astype(BF16)

    def product(j, g, at):
        return jnp.dot(xv[pl.ds(g * rows, rows), at], wgu[j, at], preferred_element_type=F32)

    def loaded(n):
        j, at = loads[n]
        with scope(f"gw{n}"):
            wait(wgu.at[j, at], local_sem.at[1 + n])

    def share(j, g, n=1):
        remote(
            hid.at[0, pl.ds(g * rows, rows), pl.ds(j * BLOCK, n * BLOCK)],
            hid.at[1, pl.ds((1 - g) * rows, rows), pl.ds(j * BLOCK, n * BLOCK)],
            ssem,
            hsem.at[g],
            {"dp": mate, "tp": tp},
        )

    whole = pl.ds(0, depth)
    with scope("xw"):
        cx.wait()
    with scope("barw"):
        pl.semaphore_wait(barrier, len(others))
    mine, theirs = pl.ds(0, rows), pl.ds(rows, rows)
    for k in (0, 1):
        remote(xv.at[mine, deep[k]], xv.at[theirs, deep[k]], ssem, xsem.at[k], {"dp": mate, "tp": tp})
    for j in range(blocks - 1):
        loaded(j)
        finish(j, 0, product(j, 0, whole))
        share(j, 0)
    loaded(blocks - 1)
    first[...] = product(blocks - 1, 0, late[0])
    loaded(blocks)
    finish(blocks - 1, 0, first[...] + product(blocks - 1, 0, late[1]))
    share(blocks - 1, 0)
    with scope("xrw0"):
        wait(xv.at[theirs, deep[0]], xsem.at[0])
    first[...] = product(0, 1, deep[0])
    with scope("xrw1"):
        wait(xv.at[theirs, deep[1]], xsem.at[1])
    finish(0, 1, first[...] + product(0, 1, deep[1]))
    for j in range(1, blocks):
        finish(j, 1, product(j, 1, whole))
    share(0, 1, blocks)

    def column(s):
        return lambda t: pl.ds(pl.multiple_of(base + s * span + t * PIECE, PIECE), PIECE)

    def start(stage, u, h):
        s, r = u // PARTS, u % PARTS
        axis = (u + h) % 2
        mine, other = pos[axis], pos[1 - axis]
        sem = rsem.at[min(stage * slices * PARTS + u, 2 * slices * PARTS) * 2 + (h if stage < 2 else 0)]
        if stage == 0:
            for d in order:
                to = lax.rem(mine + d, side)
                remote(send.at[h, u, to], part.at[h, u, d - 1], ssem, sem, peer(dp, axis, d))
        elif stage == 1:
            for d in order:
                remote(quad.at[h, u, other], quad.at[h, u, other], ssem, sem, peer(dp, 1 - axis, d))
        else:
            block = y.at[pl.ds(r * high, high), column(s)(mine)]
            if h == 0:
                for d in order:
                    remote(block, block, ssem, sem, peer(dp, axis, d))
            else:
                for d in order + (0,):
                    remote(outb.at[u], block, ssem, sem, peer(mate, axis, d))

    for h in (1, 0):
        with scope(f"hrw{h}"):
            wait(hid.at[0, pl.ds(0, rows)], hsem.at[1 - h])
        at = pl.ds(h * rows, rows)
        for s in range(slices):
            if h == 1:
                with scope(f"dw{s}"):
                    wait(wd.at[:, s], local_sem.at[2 + blocks + s])
            t = jnp.dot(hid[0, at], wd[0, s], preferred_element_type=F32)
            t = t + jnp.dot(hid[1, at], wd[1, s], preferred_element_type=F32)
            for r in range(PARTS):
                for k in range(side):
                    piece = t[r * high : (r + 1) * high, k * PIECE : (k + 1) * PIECE]
                    send[h, s * PARTS + r, k] = piece.astype(BF16)
                with scope(f"snd{h}{s}{r}"):
                    start(0, s * PARTS + r, h)
            acc[s, at] = t

    for stage in range(2):
        for h, u in [(h, u) for h in (1, 0) for u in range(slices * PARTS)]:
            s, r = u // PARTS, u % PARTS
            axis = (u + h) % 2
            mine, other = pos[axis], pos[1 - axis]
            with scope(f"rw{stage}_{u}{h}"):
                wait(part.at[h, u], rsem.at[(stage * slices * PARTS + u) * 2 + h])
            if stage == 0:
                total = acc[s, pl.ds(h * rows + r * high, high), pl.ds(pl.multiple_of(mine * PIECE, PIECE), PIECE)]
                for d in range(side - 1):
                    total = total + part[h, u, d].astype(F32)
                quad[h, u, other] = total.astype(BF16)
                start(1, u, h)
            else:
                total = quad[h, u, 0].astype(F32)
                for k in range(1, side):
                    total = total + quad[h, u, k].astype(F32)
                if h == 0:
                    y[pl.ds(r * high, high), column(s)(mine)] = total.astype(BF16)
                else:
                    outb[u] = total.astype(BF16)
                start(2, u, h)
    pieces = slices * PARTS * high * PIECE
    taken = (2 * side - 1) * pieces
    with scope("ew"):
        wait(wd.at[:, :, pl.ds(0, taken // (2 * slices * span))], rsem.at[4 * slices * PARTS])
    given = 2 * rows * half_units + rows * depth + (4 * (side - 1) + 2 * side - 1) * pieces
    with scope("sw"):
        wait(wd.at[:, :, pl.ds(0, given // (2 * slices * span))], ssem)


def solution(mesh):
    side = math.isqrt(mesh.shape["tp"])

    def step(x, w_gate, w_up, w_down):
        rows, depth = x.shape
        half_units = w_gate.shape[1] // 2
        blocks = half_units // BLOCK
        slices = depth // (2 * side * PIECE)
        count = slices * PARTS
        high = rows // PARTS
        return pl.pallas_call(
            functools.partial(_kernel, side),
            out_shape=jax.ShapeDtypeStruct((rows, depth), BF16),
            in_specs=[pl.BlockSpec(memory_space=pltpu.HBM)] * 4,
            out_specs=pl.BlockSpec(memory_space=pltpu.VMEM),
            scratch_shapes=[
                pltpu.VMEM((2 * rows, depth), BF16),
                pltpu.VMEM((blocks, depth, 2 * BLOCK), BF16),
                pltpu.VMEM((rows, 2 * BLOCK), F32),
                pltpu.VMEM((2, slices, half_units, side * PIECE), BF16),
                pltpu.VMEM((2, 2 * rows, half_units), BF16),
                pltpu.VMEM((slices, 2 * rows, side * PIECE), F32),
                pltpu.VMEM((2, count, side, high, PIECE), BF16),
                pltpu.VMEM((2, count, side - 1, high, PIECE), BF16),
                pltpu.VMEM((2, count, side, high, PIECE), BF16),
                pltpu.VMEM((count, high, PIECE), BF16),
                pltpu.SemaphoreType.DMA((2 + blocks + slices,)),
                pltpu.SemaphoreType.DMA((2,)),
                pltpu.SemaphoreType.DMA((2,)),
                pltpu.SemaphoreType.DMA,
                pltpu.SemaphoreType.DMA((4 * count + 1,)),
            ],
            compiler_params=pltpu.CompilerParams(
                collective_id=0, has_side_effects=True, vmem_limit_bytes=40 * 2**20
            ),
            name="mlp_block",
        )(*(pltpu.with_memory_space_constraint(a, pltpu.HBM) for a in (x, w_gate, w_up, w_down)))

    return jax.shard_map(
        step,
        mesh=mesh,
        in_specs=(P("dp", None), P(None, "tp"), P(None, "tp"), P("tp", None)),
        out_specs=P("dp", None),
        check_vma=False,
    )
```

```python
import contextlib
import functools
import math

import jax
import jax.numpy as jnp
from jax import lax
from jax.experimental import pallas as pl
from jax.experimental.pallas import tpu as pltpu
from jax.sharding import PartitionSpec as P

F32, BF16 = jnp.float32, jnp.bfloat16
MESH = pl.DeviceIdType.MESH
BLOCK = 256
PIECE = 128
PARTS = 2


def scope(name):
    return contextlib.nullcontext()


def _kernel(side, x_hbm, wg_hbm, wu_hbm, wd_hbm, y, xv, wgu, first, wd, hid, acc, send, part, quad, outb, local_sem, xsem, hsem, ssem, rsem):
    dp, tp = lax.axis_index("dp"), lax.axis_index("tp")
    core = lax.rem(dp, 2)
    mate = dp + 1 - 2 * core
    pos = (tp // side, lax.rem(tp, side))
    rows, depth = x_hbm.shape
    blocks = wgu.shape[0]
    half_units = blocks * BLOCK
    slices = wd.shape[1]
    span = side * PIECE
    high = rows // PARTS
    order = (2, 1, 3) if side == 4 else tuple(range(1, side))

    def peer(group, axis, d):
        p = list(pos)
        p[axis] = lax.rem(p[axis] + d, side)
        return {"dp": group, "tp": p[0] * side + p[1]}

    def remote(src, dst, send_sem, recv_sem, device):
        c = pltpu.make_async_remote_copy(
            src_ref=src, dst_ref=dst, send_sem=send_sem, recv_sem=recv_sem, device_id=device, device_id_type=MESH
        )
        c.start()

    def wait(ref, sem):
        pltpu.make_async_copy(ref, ref, sem).wait()

    barrier = pltpu.get_barrier_semaphore()
    others = [peer(mate, 0, 0)] + [peer(group, axis, d) for d in order for group in (mate, dp) for axis in (0, 1)]
    for device in others:
        pl.semaphore_signal(barrier, inc=1, device_id=device, device_id_type=MESH)

    cx = pltpu.make_async_copy(x_hbm, xv.at[pl.ds(0, rows)], local_sem.at[0])
    cx.start()
    deep = (pl.ds(0, depth // 2), pl.ds(depth // 2, depth // 2))
    cut = depth * 7 // 12
    late = (pl.ds(0, cut), pl.ds(cut, depth - cut))
    loads = [(j, pl.ds(0, depth)) for j in range(blocks - 1)] + [(blocks - 1, late[0]), (blocks - 1, late[1])]
    for n, (j, at) in enumerate(loads):
        cols = pl.ds(pl.multiple_of(core * half_units + j * BLOCK, BLOCK), BLOCK)
        for k, w in enumerate((wg_hbm, wu_hbm)):
            load = pltpu.make_async_copy(w.at[at, cols], wgu.at[j, at, pl.ds(k * BLOCK, BLOCK)], local_sem.at[1 + n])
            load.start()
    base = pl.multiple_of(core * slices * span, span)
    for s in range(slices):
        for k in (0, 1):
            units = pl.ds(pl.multiple_of((core if k == 0 else 1 - core) * half_units, BLOCK), half_units)
            cols = pl.ds(pl.multiple_of(base + s * span, span), span)
            load = pltpu.make_async_copy(wd_hbm.at[units, cols], wd.at[k, s], local_sem.at[2 + blocks + s])
            load.start()

    def finish(j, g, both):
        hidden = jax.nn.gelu(both[:, :BLOCK]) * both[:, BLOCK:]
        hid[0, pl.ds(g * rows, rows), pl.ds(j * BLOCK, BLOCK)] = hidden.astype(BF16)

    def product(j, g, at):
        return jnp.dot(xv[pl.ds(g * rows, rows), at], wgu[j, at], preferred_element_type=F32)

    def loaded(n):
        j, at = loads[n]
        with scope(f"gw{n}"):
            wait(wgu.at[j, at], local_sem.at[1 + n])

    def share(j, g, n=1):
        remote(
            hid.at[0, pl.ds(g * rows, rows), pl.ds(j * BLOCK, n * BLOCK)],
            hid.at[1, pl.ds((1 - g) * rows, rows), pl.ds(j * BLOCK, n * BLOCK)],
            ssem,
            hsem.at[g],
            {"dp": mate, "tp": tp},
        )

    whole = pl.ds(0, depth)
    with scope("xw"):
        cx.wait()
    with scope("barw"):
        pl.semaphore_wait(barrier, len(others))
    mine, theirs = pl.ds(0, rows), pl.ds(rows, rows)
    for k in (0, 1):
        remote(xv.at[mine, deep[k]], xv.at[theirs, deep[k]], ssem, xsem.at[k], {"dp": mate, "tp": tp})
    for j in range(blocks - 1):
        loaded(j)
        finish(j, 0, product(j, 0, whole))
        share(j, 0)
    loaded(blocks - 1)
    first[...] = product(blocks - 1, 0, late[0])
    loaded(blocks)
    finish(blocks - 1, 0, first[...] + product(blocks - 1, 0, late[1]))
    share(blocks - 1, 0)
    with scope("xrw0"):
        wait(xv.at[theirs, deep[0]], xsem.at[0])
    first[...] = product(0, 1, deep[0])
    with scope("xrw1"):
        wait(xv.at[theirs, deep[1]], xsem.at[1])
    finish(0, 1, first[...] + product(0, 1, deep[1]))
    for j in range(1, blocks):
        finish(j, 1, product(j, 1, whole))
    share(0, 1, blocks)

    def column(s):
        return lambda t: pl.ds(pl.multiple_of(base + s * span + t * PIECE, PIECE), PIECE)

    def start(stage, u, h):
        s, r = u // PARTS, u % PARTS
        axis = (u + h + 1) % 2
        mine, other = pos[axis], pos[1 - axis]
        sem = rsem.at[min(stage * slices + s, 2 * slices) * 2 + (h if stage < 2 else 0)]
        if stage == 0:
            for d in order:
                to = lax.rem(mine + d, side)
                remote(send.at[h, u, to], part.at[h, u, d - 1], ssem, sem, peer(dp, axis, d))
        elif stage == 1:
            for d in order:
                remote(quad.at[h, u, other], quad.at[h, u, other], ssem, sem, peer(dp, 1 - axis, d))
        else:
            block = y.at[pl.ds(r * high, high), column(s)(mine)]
            if h == 0:
                for d in order:
                    remote(block, block, ssem, sem, peer(dp, axis, d))
            else:
                for d in order + (0,):
                    remote(outb.at[u], block, ssem, sem, peer(mate, axis, d))

    for h in (1, 0):
        with scope(f"hrw{h}"):
            wait(hid.at[0, pl.ds(0, rows)], hsem.at[1 - h])
        at = pl.ds(h * rows, rows)
        for s in range(slices):
            if h == 1:
                with scope(f"dw{s}"):
                    wait(wd.at[:, s], local_sem.at[2 + blocks + s])
            t = jnp.dot(hid[0, at], wd[0, s], preferred_element_type=F32)
            t = t + jnp.dot(hid[1, at], wd[1, s], preferred_element_type=F32)
            for r in range(PARTS):
                for k in range(side):
                    piece = t[r * high : (r + 1) * high, k * PIECE : (k + 1) * PIECE]
                    send[h, s * PARTS + r, k] = piece.astype(BF16)
                with scope(f"snd{h}{s}{r}"):
                    start(0, s * PARTS + r, h)
            acc[s, at] = t

    for stage in range(2):
        for h, u in [(h, u) for h in (1, 0) for u in range(slices * PARTS)]:
            s, r = u // PARTS, u % PARTS
            axis = (u + h + 1) % 2
            mine, other = pos[axis], pos[1 - axis]
            if r == 0:
                with scope(f"rw{stage}_{s}{h}"):
                    wait(part.at[h, pl.ds(u, PARTS)], rsem.at[(stage * slices + s) * 2 + h])
            if stage == 0:
                total = acc[s, pl.ds(h * rows + r * high, high), pl.ds(pl.multiple_of(mine * PIECE, PIECE), PIECE)]
                for d in range(side - 1):
                    total = total + part[h, u, d].astype(F32)
                quad[h, u, other] = total.astype(BF16)
                start(1, u, h)
            else:
                total = quad[h, u, 0].astype(F32)
                for k in range(1, side):
                    total = total + quad[h, u, k].astype(F32)
                if h == 0:
                    y[pl.ds(r * high, high), column(s)(mine)] = total.astype(BF16)
                else:
                    outb[u] = total.astype(BF16)
                start(2, u, h)
    pieces = slices * PARTS * high * PIECE
    taken = (2 * side - 1) * pieces
    with scope("ew"):
        wait(wd.at[:, :, pl.ds(0, taken // (2 * slices * span))], rsem.at[4 * slices])
    given = 2 * rows * half_units + rows * depth + (4 * (side - 1) + 2 * side - 1) * pieces
    with scope("sw"):
        wait(wd.at[:, :, pl.ds(0, given // (2 * slices * span))], ssem)


def solution(mesh):
    side = math.isqrt(mesh.shape["tp"])

    def step(x, w_gate, w_up, w_down):
        rows, depth = x.shape
        half_units = w_gate.shape[1] // 2
        blocks = half_units // BLOCK
        slices = depth // (2 * side * PIECE)
        count = slices * PARTS
        high = rows // PARTS
        return pl.pallas_call(
            functools.partial(_kernel, side),
            out_shape=jax.ShapeDtypeStruct((rows, depth), BF16),
            in_specs=[pl.BlockSpec(memory_space=pltpu.HBM)] * 4,
            out_specs=pl.BlockSpec(memory_space=pltpu.VMEM),
            scratch_shapes=[
                pltpu.VMEM((2 * rows, depth), BF16),
                pltpu.VMEM((blocks, depth, 2 * BLOCK), BF16),
                pltpu.VMEM((rows, 2 * BLOCK), F32),
                pltpu.VMEM((2, slices, half_units, side * PIECE), BF16),
                pltpu.VMEM((2, 2 * rows, half_units), BF16),
                pltpu.VMEM((slices, 2 * rows, side * PIECE), F32),
                pltpu.VMEM((2, count, side, high, PIECE), BF16),
                pltpu.VMEM((2, count, side - 1, high, PIECE), BF16),
                pltpu.VMEM((2, count, side, high, PIECE), BF16),
                pltpu.VMEM((count, high, PIECE), BF16),
                pltpu.SemaphoreType.DMA((2 + blocks + slices,)),
                pltpu.SemaphoreType.DMA((2,)),
                pltpu.SemaphoreType.DMA((2,)),
                pltpu.SemaphoreType.DMA,
                pltpu.SemaphoreType.DMA((4 * slices + 1,)),
            ],
            compiler_params=pltpu.CompilerParams(
                collective_id=0, has_side_effects=True, vmem_limit_bytes=40 * 2**20
            ),
            name="mlp_block",
        )(*(pltpu.with_memory_space_constraint(a, pltpu.HBM) for a in (x, w_gate, w_up, w_down)))

    return jax.shard_map(
        step,
        mesh=mesh,
        in_specs=(P("dp", None), P(None, "tp"), P(None, "tp"), P("tp", None)),
        out_specs=P("dp", None),
        check_vma=False,
    )
```
